32 devices in a mesh: cfg: 8 (over z, y), lat: 4 (over x, core).
Axes of the slice: x: 2, y: 2, z: 4, core: 2. Of those that a mesh axis runs over, the one named last changes fastest.
Arguments:
- latent_mode: float32 [16, 131072], P('cfg', 'lat'), may hold values from -6 to 6
- latent_var: float32 [16, 131072], P('cfg', 'lat'), may hold values from 0.05 to 2
- config_weight: float32 [16], P('cfg'), may hold values from 0.05 to 20
- grid_offset: float32 [64], replicated, may hold values from -3 to 3
Outputs:
- marginal_density: float32 [64, 131072], P(None, ('cfg', 'lat'))
- marginal_moments: float32 [2, 131072], P(None, ('cfg', 'lat'))
The draws below stay inside these ranges and needn't reach their ends.
All inputs are finite; a program needn't handle non-finite values.
Results may differ from the reference program's by a relative error of at most 0.00002.
Values sent between devices are 32-bit elements; how exact they have to be, the bound alone decides.
A program may use at most 64 MiB of HBM per device.

```python
import math
import jax
import jax.numpy as jnp
from jax import lax

G = 64
K = 16
NLAT = 131072


def shard_levels(stream_key, dims, cuts, low, top_value):
    def one(dim, parts):
        steps = jax.random.uniform(jax.random.fold_in(jax.random.fold_in(stream_key, 6), dim), (parts,), jnp.float32, low / len(cuts), top_value / len(cuts))
        return jnp.repeat(jnp.exp(steps), dims[dim] // parts).reshape((-1,) + (1,) * (len(dims) - dim - 1))

    factor_of = one(*cuts[0])
    for cut in cuts[1:]:
        factor_of = factor_of * one(*cut)
    return factor_of


def scatter_about(own_key, dims, scale, limit, cuts=(), held_as=jnp.bfloat16):
    result = jax.random.normal(own_key, dims, jnp.float32) * scale
    if len(cuts) > 0:
        result = shard_levels(own_key, dims, cuts, -0.22, 0.18) * result
    return jnp.clip(result, min=-limit, max=limit).astype(held_as)


def setup_inputs(seed: int = 0) -> dict:
    key_of = jax.random.split(jax.random.key(seed), 5)
    latent_mode = scatter_about(key_of[0], (K, NLAT), 1.0, 6.0, ((0, 8), (1, 4)), jnp.float32)
    latent_var = jnp.clip(jnp.exp(math.log(2.0) - 3.6888794 * jax.random.uniform(key_of[1], (K, NLAT), jnp.float32) ** shard_levels(key_of[1], (K, NLAT), ((0, 8), (1, 4)), -0.2, 0.2)), 0.05, 2.0)
    config_weight = jnp.clip(jnp.exp(math.log(20.0) - 5.9914645 * jax.random.uniform(key_of[2], (K,), jnp.float32) ** shard_levels(key_of[2], (K,), ((0, 8),), -0.2, 0.2)), 0.05, 20.0)
    grid_offset = jnp.clip(jax.random.uniform(key_of[3], (G,), jnp.float32, -3.0, 3.0), -3.0, 3.0)
    return {"latent_mode": latent_mode, "latent_var": latent_var, "config_weight": config_weight, "grid_offset": grid_offset}


def mixture(mode_block, var_block, norm_weight, grid_offset):
    centre = lax.optimization_barrier(jnp.sum(norm_weight[:, None] * mode_block, axis=0))
    deviation = mode_block - centre[None, :]
    spread = jnp.sqrt(lax.optimization_barrier(jnp.sum(norm_weight[:, None] * (var_block + deviation * deviation), axis=0)))
    points = centre[None, :] + grid_offset[:, None] * spread[None, :]
    coefficient = norm_weight[:, None] / jnp.sqrt(6.283185307179586 * var_block)
    precision = 1.0 / var_block
    gap = points[None, :, :] - mode_block[:, None, :]
    terms = coefficient[:, None, :] * jnp.exp(-0.5 * gap * gap * precision[:, None, :])
    density = spread[None, :] * lax.optimization_barrier(jnp.sum(terms, axis=0))
    return (density, jnp.stack([centre, spread], axis=0))

def reference(latent_mode, latent_var, config_weight, grid_offset):
    norm_weight = config_weight / jnp.sum(config_weight)
    width = min(NLAT, 4096)
    count = NLAT // width
    modes_blocked = latent_mode.reshape(K, count, width).transpose(1, 0, 2)
    vars_blocked = latent_var.reshape(K, count, width).transpose(1, 0, 2)

    def one_block(pair):
        return mixture(pair[0], pair[1], norm_weight, grid_offset)
    density, moments = lax.map(one_block, (modes_blocked, vars_blocked))
    density = density.transpose(1, 0, 2).reshape(G, NLAT)
    moments = moments.transpose(1, 0, 2).reshape(2, NLAT)
    return (density, moments)
```

```python
import functools
import math

import jax
import jax.numpy as jnp
from jax import lax
from jax.experimental import pallas as pl
from jax.experimental.pallas import tpu as pltpu
from jax.sharding import PartitionSpec as P

LANES = 128
CORES = 2
FAR = 0
AHEAD = 2
MESH = pl.DeviceIdType.MESH
HALF_LOG2E = 0.5 * math.log2(math.e)
TWO_PI = 6.283185307179586


def over(n, body, init):
    if n <= 16:
        for i in range(n):
            init = body(i, init)
        return init
    return lax.fori_loop(0, n, body, init)


def densities(grid_col, rows_u, rows_v, rows_c, out_ref, first):
    n_config, tiles, _ = rows_u.shape
    grid = grid_col[...]

    def one_tile(t, carry):
        def term(k, acc):
            at = grid * rows_u[k, pl.ds(t, 1), :] + rows_v[k, pl.ds(t, 1), :]
            return acc + jnp.exp2(rows_c[k, pl.ds(t, 1), :] - at * at)

        acc = over(n_config, term, jnp.zeros(grid.shape, jnp.float32))
        column_at = pl.multiple_of((first + t) * LANES, LANES)
        out_ref[:, pl.ds(column_at, LANES)] = acc
        return carry

    lax.fori_loop(0, tiles, one_tile, 0)


def kernel(
    n_cfg, n_lat, own, n_chunk, n_far, tiles,
    mode_ref, var_ref, weight_hbm, grid_hbm,
    density_ref, moments_ref, rows_u, rows_v, rows_c, grid_col,
    stage, relay, landed, weights, norm, weight_ref, grid_ref,
    small_sem, go_sem, load_sem, pass_sem, relay_sem, far_sem, send_sem, recv_sem, wsend_sem, wrecv_sem,
):
    my_cfg = lax.axis_index("cfg")
    my_lat = lax.axis_index("lat")
    me = my_cfg * n_lat + my_lat
    n_group = n_lat // CORES
    group, core = my_lat // CORES, lax.rem(my_lat, CORES)
    n_config = n_cfg * own
    per_group = n_cfg // n_group

    def load(step, chunk):
        to = lax.rem(group + step, n_group)
        for a, ref in enumerate((mode_ref, var_ref)):
            pltpu.make_async_copy(
                ref.at[:, to, :, chunk], stage.at[to, chunk, :, :, a],
                load_sem.at[step, chunk],
            ).start()

    barrier = pltpu.get_barrier_semaphore()
    gate = CORES - 1

    for step in range(1, n_group):
        peer = lax.rem(group + step, n_group) * CORES + core
        pl.semaphore_signal(
            barrier, inc=1, device_id=(my_cfg, peer), device_id_type=MESH
        )

    def greet(i, carry):
        @pl.when(jnp.logical_or(i != my_cfg, core != gate))
        def _():
            pl.semaphore_signal(
                barrier, inc=1, device_id=(i, group * CORES + gate), device_id_type=MESH
            )
        return carry

    over(n_cfg, greet, 0)

    for chunk in range(n_chunk):
        for step in range(1, n_group):
            load(step, chunk)
    for chunk in range(n_chunk):
        load(0, chunk)
    small = [
        pltpu.make_async_copy(weight_hbm, weight_ref, small_sem.at[0]),
        pltpu.make_async_copy(grid_hbm, grid_ref, small_sem.at[1]),
    ]
    for copy in small:
        copy.start()

    everyone = n_group - 1 + n_cfg * CORES - 1
    pl.semaphore_wait(barrier, jnp.where(core == gate, everyone, n_group - 1))

    @pl.when(core == gate)
    def _():
        for other in range(CORES - 1):
            pl.semaphore_signal(
                go_sem, inc=1, device_id=(my_cfg, group * CORES + other), device_id_type=MESH
            )

    def loaded(step, chunk):
        to = lax.rem(group + step, n_group)
        block = stage.at[to, chunk]
        pltpu.make_async_copy(block, block, load_sem.at[step, chunk]).wait()

    n_a = n_cfg // n_lat
    n_part = 2 if n_a % 2 == 0 else 1
    size = n_a // n_part
    pieces = [(chunk, part) for chunk in range(n_chunk) for part in range(n_part)]
    passed = pieces[:len(pieces) - n_far] if n_far else pieces

    for chunk, part in pieces:
        for step in range(1, n_group):
            to = lax.rem(group + step, n_group)
            if part == 0:
                loaded(step, chunk)
            if (chunk, part) in passed:
                span = pl.ds(part * size, size)
                pltpu.make_async_remote_copy(
                    src_ref=stage.at[to, chunk, span],
                    dst_ref=relay.at[group, chunk, span],
                    send_sem=pass_sem.at[to, part],
                    recv_sem=relay_sem.at[group, chunk, part],
                    device_id=(my_cfg, to * CORES + core), device_id_type=MESH,
                ).start()

    def target(origin, i, to=group):
        slot = (i // CORES) * n_lat + to * CORES + i % CORES
        flat = (origin * CORES + core) * n_cfg + slot
        return flat, (flat // n_lat, lax.rem(flat, n_lat))

    def send_weights(origin):
        def send(i, carry):
            flat, device = target(origin, i)

            @pl.when(flat == me)
            def _():
                pltpu.make_async_copy(weight_ref, weights.at[my_cfg], wrecv_sem).start()

            @pl.when(flat != me)
            def _():
                pltpu.make_async_remote_copy(
                    src_ref=weight_ref, dst_ref=weights.at[my_cfg],
                    send_sem=wsend_sem.at[origin, i], recv_sem=wrecv_sem,
                    device_id=device, device_id_type=MESH,
                ).start()
            return carry

        over(per_group, send, 0)

    def send_blocks(origin, source, chunk, part):
        def send(i, carry):
            i = i + part * size * CORES
            flat, device = target(origin, i)
            src = source.at[i // CORES, i % CORES]
            dst = landed.at[chunk, my_cfg]

            @pl.when(flat == me)
            def _():
                pltpu.make_async_copy(src, dst, recv_sem.at[chunk]).start()

            @pl.when(flat != me)
            def _():
                pltpu.make_async_remote_copy(
                    src_ref=src, dst_ref=dst,
                    send_sem=send_sem.at[origin, i], recv_sem=recv_sem.at[chunk],
                    device_id=device, device_id_type=MESH,
                ).start()
            return carry

        over(size * CORES, send, 0)

    def send_far(step, chunk, part):
        to = lax.rem(group + step, n_group)

        def send(i, carry):
            i = i + part * size * CORES
            _, device = target(group, i, to)
            pltpu.make_async_remote_copy(
                src_ref=stage.at[to, chunk, i // CORES, i % CORES],
                dst_ref=landed.at[chunk, my_cfg],
                send_sem=far_sem.at[to, chunk, i], recv_sem=recv_sem.at[chunk],
                device_id=device, device_id_type=MESH,
            ).start()
            return carry

        over(size * CORES, send, 0)

    def send_own(chunk):
        loaded(0, chunk)
        for part in range(n_part):
            send_blocks(group, stage.at[group, chunk], chunk, part)

    @pl.when(core != gate)
    def _():
        pl.semaphore_wait(go_sem, 1)

    small[0].wait()
    ahead = min(AHEAD, n_chunk)
    for chunk in range(ahead):
        send_own(chunk)
        if chunk == 0:
            for step in range(n_group):
                send_weights(lax.rem(group + step, n_group))
    for chunk, part in pieces:
        for step in range(1, n_group):
            origin = lax.rem(group + step, n_group)
            if (chunk, part) in passed:
                block = relay.at[origin, chunk, pl.ds(part * size, size)]
                pltpu.make_async_copy(
                    block, block, relay_sem.at[origin, chunk, part]
                ).wait()
                send_blocks(origin, relay.at[origin, chunk], chunk, part)
            else:
                send_far(step, chunk, part)
        if part == n_part - 1 and chunk + ahead < n_chunk:
            send_own(chunk + ahead)

    small[1].wait()
    points = grid_ref.shape[1]
    on_diagonal = lax.broadcasted_iota(jnp.int32, (points, points), 0) == lax.broadcasted_iota(
        jnp.int32, (points, points), 1
    )
    column = jnp.sum(jnp.where(on_diagonal, grid_ref[...], 0.0), axis=1, keepdims=True)
    grid_col[...] = jnp.broadcast_to(column, (points, LANES))

    pltpu.make_async_copy(weights, weights, wrecv_sem).wait()
    total = jnp.zeros((1, 1), jnp.float32)
    for c in range(n_cfg):
        total = total + jnp.sum(weights[c], axis=1, keepdims=True)
    for c in range(n_cfg):
        scaled = weights[c] / total
        for j in range(own):
            norm[c * own + j] = jnp.broadcast_to(scaled[:, j:j + 1], (1, LANES))

    def drain_all():
        def spent(block, sem):
            pltpu.make_async_copy(block, block, sem).wait()

        for step in range(n_group):
            origin = lax.rem(group + step, n_group)

            def drain(i, carry):
                flat, _ = target(origin, i)

                @pl.when(flat != me)
                def _():
                    spent(weight_ref, wsend_sem.at[origin, i])

                def drain_blocks(n):
                    @pl.when(flat != me)
                    def _():
                        spent(landed.at[pl.ds(0, n), 0], send_sem.at[origin, i])

                part = i // (CORES * size)
                if step == 0 or not n_far:
                    drain_blocks(n_chunk)
                else:
                    for p in range(n_part):
                        n = sum(1 for _, q in passed if q == p)
                        if n:
                            pl.when(part == p)(functools.partial(drain_blocks, n))
                return carry

            over(per_group, drain, 0)

            if step:
                for part in range(n_part):
                    pieces_sent = [chunk for chunk, q in passed if q == part]
                    span = pl.ds(part * size, size)
                    if pieces_sent:
                        spent(stage.at[origin, pl.ds(0, len(pieces_sent)), span],
                              pass_sem.at[origin, part])
                for chunk, part in pieces[len(passed):]:
                    def drain_far(i, carry):
                        spent(landed.at[0, 0], far_sem.at[origin, chunk, i])
                        return carry
                    if size * CORES <= 16:
                        for i in range(size * CORES):
                            drain_far(i + part * size * CORES, 0)
                    else:
                        lax.fori_loop(part * size * CORES, (part + 1) * size * CORES, drain_far, 0)

    shape = (tiles, LANES)
    for chunk in range(n_chunk):
        if chunk == n_chunk - 1:
            drain_all()
        pltpu.make_async_copy(landed.at[chunk], landed.at[chunk], recv_sem.at[chunk]).wait()

        def value(c, a, j):
            return landed[chunk, c, a, pl.ds(j, tiles, stride=own), :]

        def add_mode(c, acc):
            for j in range(own):
                acc = acc + norm[c * own + j] * value(c, 0, j)
            return acc

        centre = over(n_cfg, add_mode, jnp.zeros(shape, jnp.float32))

        def add_var(c, acc):
            for j in range(own):
                off = value(c, 0, j) - centre
                acc = acc + norm[c * own + j] * (value(c, 1, j) + off * off)
            return acc

        spread = jnp.sqrt(over(n_cfg, add_var, jnp.zeros(shape, jnp.float32)))
        moments_ref[pl.ds(2 * tiles * chunk, tiles, stride=2), :] = centre
        moments_ref[pl.ds(2 * tiles * chunk + 1, tiles, stride=2), :] = spread

        def prepare(c, carry):
            for j in range(own):
                k = c * own + j
                root = lax.rsqrt(value(c, 1, j))
                scale = root * math.sqrt(HALF_LOG2E)
                rows_u[k] = spread * scale
                rows_v[k] = (centre - value(c, 0, j)) * scale
                rows_c[k] = jnp.log2(norm[k] * spread * root * (1.0 / math.sqrt(TWO_PI)))
            return carry

        over(n_cfg, prepare, 0)

        if chunk < n_chunk - 1:
            densities(
                grid_col, rows_u, rows_v, rows_c, density_ref, chunk * tiles
            )


def finish(
    n_chunk, tiles,
    done_ref, made_ref, rows_u, rows_v, rows_c, grid_col,
    density_ref, moments_ref,
    last, sems,
):
    early = done_ref.shape[1]
    copies = [
        pltpu.make_async_copy(done_ref, density_ref.at[:, pl.ds(0, early)], sems.at[0]),
        pltpu.make_async_copy(made_ref, moments_ref, sems.at[1]),
    ]
    for copy in copies:
        copy.start()
    densities(grid_col, rows_u, rows_v, rows_c, last, 0)
    copies.append(
        pltpu.make_async_copy(
            last, density_ref.at[:, pl.ds(early, tiles * LANES)], sems.at[2]
        )
    )
    copies[2].start()
    for copy in copies:
        copy.wait()


def interleave(block, n_cfg, n_lat, n_chunk):
    own, columns = block.shape
    rows = block.reshape(own, columns // LANES, LANES).transpose(1, 0, 2)
    n_row = columns * own // (LANES * n_cfg * n_chunk)
    return rows.reshape(n_cfg // n_lat, n_lat // CORES, CORES, n_chunk, n_row, LANES)


def per_device(latent_mode, latent_var, config_weight, grid_offset):
    n_cfg = lax.axis_size("cfg")
    n_lat = lax.axis_size("lat")
    own, columns = latent_mode.shape
    lat_dev = columns // n_cfg
    points = grid_offset.shape[0]
    n_chunk = 4
    n_far = FAR
    tiles = lat_dev // (LANES * n_chunk)
    n_config = own * n_cfg
    n_group = n_lat // CORES
    per_group = n_cfg // n_group
    passing = (n_group, n_chunk, n_cfg // n_lat, CORES, 2, own * tiles, LANES)
    f32 = jnp.float32
    hbm = pl.BlockSpec(memory_space=pl.ANY)
    vmem = pl.BlockSpec(memory_space=pltpu.VMEM)
    early = lat_dev - tiles * LANES
    interleaved = (2 * lat_dev // LANES, LANES)
    rows = (n_config, tiles, LANES)
    parts = pl.pallas_call(
        functools.partial(kernel, n_cfg, n_lat, own, n_chunk, n_far, tiles),
        out_shape=(
            pltpu.VMEM((points, early), f32),
            pltpu.VMEM(interleaved, f32),
            pltpu.VMEM(rows, f32),
            pltpu.VMEM(rows, f32),
            pltpu.VMEM(rows, f32),
            pltpu.VMEM((points, LANES), f32),
        ),
        in_specs=[hbm, hbm, hbm, hbm],
        out_specs=(vmem,) * 6,
        scratch_shapes=[
            pltpu.VMEM(passing, f32),
            pltpu.VMEM(passing, f32),
            pltpu.VMEM((n_chunk, n_cfg, 2, own * tiles, LANES), f32),
            pltpu.VMEM((n_cfg, 1, own), f32),
            pltpu.VMEM((n_config, 1, LANES), f32),
            pltpu.VMEM((1, own), f32),
            pltpu.VMEM((1, points), f32),
            pltpu.SemaphoreType.DMA((2,)),
            pltpu.SemaphoreType.REGULAR,
            pltpu.SemaphoreType.DMA((n_group, n_chunk)),
            pltpu.SemaphoreType.DMA((n_group, 2)),
            pltpu.SemaphoreType.DMA((n_group, n_chunk, 2)),
            pltpu.SemaphoreType.DMA((n_group, n_chunk, per_group)),
            pltpu.SemaphoreType.DMA((n_group, per_group)),
            pltpu.SemaphoreType.DMA((n_chunk,)),
            pltpu.SemaphoreType.DMA((n_group, per_group)),
            pltpu.SemaphoreType.DMA,
        ],
        compiler_params=pltpu.CompilerParams(collective_id=0, has_side_effects=True),
    )(
        interleave(latent_mode, n_cfg, n_lat, n_chunk),
        interleave(latent_var, n_cfg, n_lat, n_chunk),
        config_weight.reshape(1, own),
        grid_offset.reshape(1, points),
    )
    density, moments = pl.pallas_call(
        functools.partial(finish, n_chunk, tiles),
        out_shape=(
            jax.ShapeDtypeStruct((points, lat_dev), f32),
            jax.ShapeDtypeStruct(interleaved, f32),
        ),
        in_specs=[vmem] * 6,
        out_specs=(hbm, hbm),
        scratch_shapes=[
            pltpu.VMEM((points, tiles * LANES), f32),
            pltpu.SemaphoreType.DMA((3,)),
        ],
    )(*(pltpu.with_memory_space_constraint(part, pltpu.VMEM) for part in parts))
    moments = moments.reshape(lat_dev // LANES, 2, LANES).transpose(1, 0, 2).reshape(2, lat_dev)
    return (density, moments)


def solution(mesh):
    return jax.shard_map(
        per_device,
        mesh=mesh,
        in_specs=(P("cfg", "lat"), P("cfg", "lat"), P("cfg"), P()),
        out_specs=(P(None, ("cfg", "lat")), P(None, ("cfg", "lat"))),
        check_vma=False,
    )
```

```python
import functools
import math

import jax
import jax.numpy as jnp
from jax import lax
from jax.experimental import pallas as pl
from jax.experimental.pallas import tpu as pltpu
from jax.sharding import PartitionSpec as P

LANES = 128
CORES = 2
UNITS = (2, 2, 2, 1, 1)
AHEAD = 2
HOPS = 5
MESH = pl.DeviceIdType.MESH
HALF_LOG2E = 0.5 * math.log2(math.e)
TWO_PI = 6.283185307179586


def over(n, body, init):
    if n <= 16:
        for i in range(n):
            init = body(i, init)
        return init
    return lax.fori_loop(0, n, body, init)


def densities(grid_col, rows_u, rows_v, rows_c, tiles, out_ref, first):
    n_config = rows_u.shape[0]
    grid = grid_col[...]

    def one_tile(t, carry):
        def term(k, acc):
            at = grid * rows_u[k, pl.ds(t, 1), :] + rows_v[k, pl.ds(t, 1), :]
            return acc + jnp.exp2(rows_c[k, pl.ds(t, 1), :] - at * at)

        acc = over(n_config, term, jnp.zeros(grid.shape, jnp.float32))
        column_at = pl.multiple_of((first + t) * LANES, LANES)
        out_ref[:, pl.ds(column_at, LANES)] = acc
        return carry

    lax.fori_loop(0, tiles, one_tile, 0)


def kernel(
    n_cfg, n_lat, own, spans,
    mode_ref, var_ref, weight_hbm, grid_hbm,
    density_ref, moments_ref, last_u, last_v, last_c, grid_col,
    stage, relay, landed, weights, norm, weight_ref, grid_ref, rows_u, rows_v, rows_c,
    small_sem, go_sem, rest_sem, load_sem, pass_sem, relay_sem, send_sem, recv_sem, wsend_sem, wrecv_sem,
):
    my_cfg = lax.axis_index("cfg")
    my_lat = lax.axis_index("lat")
    me = my_cfg * n_lat + my_lat
    n_group = n_lat // CORES
    group, core = my_lat // CORES, lax.rem(my_lat, CORES)
    per_group = n_cfg // n_group
    n_chunk = len(spans)

    def rows_of(chunk, until=None):
        start = 2 * own * spans[chunk][0]
        t, n = spans[chunk if until is None else until]
        return pl.ds(start, 2 * own * (t + n) - start)

    barrier = pltpu.get_barrier_semaphore()
    half_cfg = n_cfg // 2
    half = my_cfg // half_cfg
    gate = 1 - half
    is_gate = core == gate

    for step in range(1, n_group):
        peer = lax.rem(group + step, n_group) * CORES + core
        pl.semaphore_signal(
            barrier, inc=1, device_id=(my_cfg, peer), device_id_type=MESH
        )

    def greet(i, carry):
        early = i < half_cfg
        mate = jnp.logical_and(i == my_cfg, core != gate)
        others = jnp.logical_and(i != my_cfg, jnp.logical_or(early, half == 0))

        @pl.when(jnp.logical_or(mate, others))
        def _():
            pl.semaphore_signal(
                barrier, inc=1,
                device_id=(i, group * CORES + jnp.where(early, 1, 0)), device_id_type=MESH,
            )
        return carry

    over(n_cfg, greet, 0)

    for chunk in range(n_chunk):
        start, tiles = spans[chunk]
        n_row = own * tiles
        for step in list(range(1, n_group)) + [0]:
            to = lax.rem(group + step, n_group)
            for a, ref in enumerate((mode_ref, var_ref)):
                pltpu.make_async_copy(
                    ref.at[:, to, :, pl.ds(own * start, n_row)],
                    stage.at[to, :, :, pl.ds(2 * own * start + a * n_row, n_row)],
                    load_sem.at[step, min(chunk, 1)],
                ).start()
    small = [
        pltpu.make_async_copy(weight_hbm, weight_ref, small_sem.at[0]),
        pltpu.make_async_copy(grid_hbm, grid_ref, small_sem.at[1]),
    ]
    for copy in small:
        copy.start()

    peers = n_group - 1
    gathered = jnp.where(half == 0, n_cfg * CORES - 1, half_cfg * CORES + 1)
    pl.semaphore_wait(barrier, peers + jnp.where(is_gate, gathered, 0))

    @pl.when(is_gate)
    def _():
        pl.semaphore_signal(
            go_sem, inc=1, device_id=(my_cfg, group * CORES + 1 - gate), device_id_type=MESH
        )

        @pl.when(half == 0)
        def _():
            for other in range(CORES):
                pl.semaphore_signal(
                    rest_sem, inc=1,
                    device_id=(my_cfg + half_cfg, group * CORES + other), device_id_type=MESH,
                )

    def spent(block, sem):
        pltpu.make_async_copy(block, block, sem).wait()

    def loaded(step, chunk):
        to = lax.rem(group + step, n_group)
        if chunk == 0:
            spent(stage.at[to, :, :, rows_of(0)], load_sem.at[step, 0])
        if chunk == 1:
            spent(stage.at[to, :, :, rows_of(1, n_chunk - 1)], load_sem.at[step, 1])

    def hop(chunk):
        for step in range(1, n_group):
            to = lax.rem(group + step, n_group)
            loaded(step, chunk)
            slot = n_group - step - 1
            pltpu.make_async_remote_copy(
                src_ref=stage.at[to, :, :, rows_of(chunk)],
                dst_ref=relay.at[slot, :, :, rows_of(chunk)],
                send_sem=pass_sem, recv_sem=relay_sem.at[slot, chunk],
                device_id=(my_cfg, to * CORES + core), device_id_type=MESH,
            ).start()

    hops = min(HOPS, n_chunk)
    for chunk in range(hops):
        hop(chunk)

    @pl.when(jnp.logical_not(is_gate))
    def _():
        pl.semaphore_wait(go_sem, 1)

    for chunk in range(hops, n_chunk):
        hop(chunk)

    def target(origin, i):
        slot = (i // CORES) * n_lat + group * CORES + i % CORES
        flat = (origin * CORES + core) * n_cfg + slot
        return flat, (flat // n_lat, lax.rem(flat, n_lat))

    def send_weights(origin):
        def send(i, carry):
            flat, device = target(origin, i)

            @pl.when(flat == me)
            def _():
                pltpu.make_async_copy(weight_ref, weights.at[my_cfg], wrecv_sem).start()

            @pl.when(flat != me)
            def _():
                pltpu.make_async_remote_copy(
                    src_ref=weight_ref, dst_ref=weights.at[my_cfg],
                    send_sem=wsend_sem, recv_sem=wrecv_sem,
                    device_id=device, device_id_type=MESH,
                ).start()
            return carry

        over(per_group, send, 0)

    def send_blocks(origin, source, chunk):
        rows = rows_of(chunk)

        def send(i, carry):
            flat, device = target(origin, i)
            src = source.at[i // CORES, i % CORES, rows]
            dst = landed.at[my_cfg, rows]

            @pl.when(flat == me)
            def _():
                pltpu.make_async_copy(src, dst, recv_sem.at[chunk]).start()

            @pl.when(flat != me)
            def _():
                pltpu.make_async_remote_copy(
                    src_ref=src, dst_ref=dst,
                    send_sem=send_sem, recv_sem=recv_sem.at[chunk],
                    device_id=device, device_id_type=MESH,
                ).start()
            return carry

        over(per_group, send, 0)

    def send_own(chunk):
        loaded(0, chunk)
        send_blocks(group, stage.at[group], chunk)

    def crosses(origin):
        return (origin * CORES + core) * 2 // n_lat != half

    def send_relayed(chunk):
        for step in range(1, n_group):
            origin = lax.rem(group + step, n_group)
            block = relay.at[step - 1, :, :, rows_of(chunk)]
            spent(block, relay_sem.at[step - 1, chunk])
            send_blocks(origin, relay.at[step - 1], chunk)

    own_first = crosses(group)

    def weights_where(first):
        for origin in range(n_group):
            @pl.when(crosses(origin) == first)
            def _():
                send_weights(origin)

    small[0].wait()
    weights_where(True)

    @pl.when(half == 0)
    def _():
        weights_where(False)

    @pl.when(jnp.logical_or(half == 0, own_first))
    def _():
        for chunk in range(n_chunk):
            send_own(chunk)

    ahead = min(AHEAD, n_chunk)

    @pl.when(jnp.logical_not(own_first))
    def _():
        for chunk in range(ahead):
            send_relayed(chunk)

    @pl.when(half == 1)
    def _():
        pl.semaphore_wait(rest_sem, 1)
        weights_where(False)

        @pl.when(jnp.logical_not(own_first))
        def _():
            for chunk in range(n_chunk):
                send_own(chunk)

    @pl.when(own_first)
    def _():
        for chunk in range(ahead):
            send_relayed(chunk)

    for chunk in range(ahead, n_chunk):
        send_relayed(chunk)

    small[1].wait()
    points = grid_ref.shape[1]
    on_diagonal = lax.broadcasted_iota(jnp.int32, (points, points), 0) == lax.broadcasted_iota(
        jnp.int32, (points, points), 1
    )
    column = jnp.sum(jnp.where(on_diagonal, grid_ref[...], 0.0), axis=1, keepdims=True)
    grid_col[...] = jnp.broadcast_to(column, (points, LANES))

    pltpu.make_async_copy(weights, weights, wrecv_sem).wait()
    total = jnp.zeros((1, 1), jnp.float32)
    for c in range(n_cfg):
        total = total + jnp.sum(weights[c], axis=1, keepdims=True)
    for c in range(n_cfg):
        scaled = weights[c] / total
        for j in range(own):
            norm[c * own + j] = jnp.broadcast_to(scaled[:, j:j + 1], (1, LANES))

    for chunk in range(n_chunk):
        start, tiles = spans[chunk]
        base = 2 * own * start
        n_row = own * tiles
        shape = (tiles, LANES)
        arrived = landed.at[:, rows_of(chunk)]
        pltpu.make_async_copy(arrived, arrived, recv_sem.at[chunk]).wait()

        def value(c, a, j):
            return landed[c, pl.ds(base + a * n_row + j, tiles, stride=own), :]

        def add_mode(c, acc):
            for j in range(own):
                acc = acc + norm[c * own + j] * value(c, 0, j)
            return acc

        centre = over(n_cfg, add_mode, jnp.zeros(shape, jnp.float32))

        def add_var(c, acc):
            for j in range(own):
                off = value(c, 0, j) - centre
                acc = acc + norm[c * own + j] * (value(c, 1, j) + off * off)
            return acc

        spread = jnp.sqrt(over(n_cfg, add_var, jnp.zeros(shape, jnp.float32)))
        moments_ref[pl.ds(2 * start, tiles, stride=2), :] = centre
        moments_ref[pl.ds(2 * start + 1, tiles, stride=2), :] = spread

        final = chunk == n_chunk - 1
        to_u, to_v, to_c = (last_u, last_v, last_c) if final else (rows_u, rows_v, rows_c)

        def prepare(c, carry):
            for j in range(own):
                k = c * own + j
                root = lax.rsqrt(value(c, 1, j))
                scale = root * math.sqrt(HALF_LOG2E)
                to_u[k, pl.ds(0, tiles)] = spread * scale
                to_v[k, pl.ds(0, tiles)] = (centre - value(c, 0, j)) * scale
                to_c[k, pl.ds(0, tiles)] = jnp.log2(
                    norm[k] * spread * root * (1.0 / math.sqrt(TWO_PI))
                )
            return carry

        over(n_cfg, prepare, 0)

        if not final:
            densities(
                grid_col, rows_u, rows_v, rows_c, tiles, density_ref, start
            )

    spent(stage.at[pl.ds(0, n_group - 1)], pass_sem)
    for kept, n in ((lax.rem(me // n_cfg, CORES) == core, n_cfg - 1),
                    (lax.rem(me // n_cfg, CORES) != core, n_cfg)):
        @pl.when(kept)
        def _():
            spent(weights.at[pl.ds(0, n)], wsend_sem)
            spent(landed.at[pl.ds(0, n)], send_sem)


def finish(
    tiles,
    done_ref, made_ref, rows_u, rows_v, rows_c, grid_col,
    density_ref, moments_ref,
    last, sems,
):
    early = done_ref.shape[1]
    copies = [
        pltpu.make_async_copy(done_ref, density_ref.at[:, pl.ds(0, early)], sems.at[0]),
        pltpu.make_async_copy(made_ref, moments_ref, sems.at[1]),
    ]
    for copy in copies:
        copy.start()
    densities(grid_col, rows_u, rows_v, rows_c, tiles, last, 0)
    copies.append(
        pltpu.make_async_copy(
            last, density_ref.at[:, pl.ds(early, tiles * LANES)], sems.at[2]
        )
    )
    copies[2].start()
    for copy in copies:
        copy.wait()


def interleave(block, n_cfg, n_lat):
    own, columns = block.shape
    rows = block.reshape(own, columns // LANES, LANES).transpose(1, 0, 2)
    n_row = columns * own // (LANES * n_cfg)
    return rows.reshape(n_cfg // n_lat, n_lat // CORES, CORES, n_row, LANES)


def per_device(latent_mode, latent_var, config_weight, grid_offset):
    n_cfg = lax.axis_size("cfg")
    n_lat = lax.axis_size("lat")
    own, columns = latent_mode.shape
    lat_dev = columns // n_cfg
    points = grid_offset.shape[0]
    unit = lat_dev // (LANES * sum(UNITS))
    spans = []
    for n in UNITS:
        spans.append((sum(s[1] for s in spans), n * unit))
    most, last = max(n for _, n in spans[:-1]), spans[-1][1]
    n_chunk = len(spans)
    n_config = own * n_cfg
    n_group = n_lat // CORES
    n_row = 2 * own * lat_dev // LANES
    n_a = n_cfg // n_lat
    f32 = jnp.float32
    hbm = pl.BlockSpec(memory_space=pl.ANY)
    vmem = pl.BlockSpec(memory_space=pltpu.VMEM)
    early = lat_dev - last * LANES
    interleaved = (2 * lat_dev // LANES, LANES)
    dma = pltpu.SemaphoreType.DMA
    parts = pl.pallas_call(
        functools.partial(kernel, n_cfg, n_lat, own, spans),
        out_shape=(
            pltpu.VMEM((points, early), f32),
            pltpu.VMEM(interleaved, f32),
            pltpu.VMEM((n_config, last, LANES), f32),
            pltpu.VMEM((n_config, last, LANES), f32),
            pltpu.VMEM((n_config, last, LANES), f32),
            pltpu.VMEM((points, LANES), f32),
        ),
        in_specs=[hbm] * 4,
        out_specs=(vmem,) * 6,
        scratch_shapes=[
            pltpu.VMEM((n_group, n_a, CORES, n_row, LANES), f32),
            pltpu.VMEM((n_group - 1, n_a, CORES, n_row, LANES), f32),
            pltpu.VMEM((n_cfg, n_row, LANES), f32),
            pltpu.VMEM((n_cfg, 1, own), f32),
            pltpu.VMEM((n_config, 1, LANES), f32),
            pltpu.VMEM((1, own), f32),
            pltpu.VMEM((1, points), f32),
            pltpu.VMEM((n_config, most, LANES), f32),
            pltpu.VMEM((n_config, most, LANES), f32),
            pltpu.VMEM((n_config, most, LANES), f32),
            dma((2,)),
            pltpu.SemaphoreType.REGULAR,
            pltpu.SemaphoreType.REGULAR,
            dma((n_group, 2)),
            dma,
            dma((n_group - 1, n_chunk)),
            dma,
            dma((n_chunk,)),
            dma,
            dma,
        ],
        compiler_params=pltpu.CompilerParams(collective_id=0, has_side_effects=True),
    )(
        interleave(latent_mode, n_cfg, n_lat),
        interleave(latent_var, n_cfg, n_lat),
        config_weight.reshape(1, own),
        grid_offset.reshape(1, points),
    )
    density, moments = pl.pallas_call(
        functools.partial(finish, last),
        out_shape=(
            jax.ShapeDtypeStruct((points, lat_dev), f32),
            jax.ShapeDtypeStruct(interleaved, f32),
        ),
        in_specs=[vmem] * 6,
        out_specs=(hbm, hbm),
        scratch_shapes=[
            pltpu.VMEM((points, last * LANES), f32),
            dma((3,)),
        ],
    )(*(pltpu.with_memory_space_constraint(part, pltpu.VMEM) for part in parts))
    moments = moments.reshape(lat_dev // LANES, 2, LANES).transpose(1, 0, 2).reshape(2, lat_dev)
    return (density, moments)


def solution(mesh):
    return jax.shard_map(
        per_device,
        mesh=mesh,
        in_specs=(P("cfg", "lat"), P("cfg", "lat"), P("cfg"), P()),
        out_specs=(P(None, ("cfg", "lat")), P(None, ("cfg", "lat"))),
        check_vma=False,
    )
```

```python
import functools
import math

import jax
import jax.numpy as jnp
from jax import lax
from jax.experimental import pallas as pl
from jax.experimental.pallas import tpu as pltpu
from jax.sharding import PartitionSpec as P

LANES = 128
CORES = 2
UNITS = (1, 1, 1, 1, 1, 1, 1, 1)
AHEAD = 4
LEAD = 4
HOLD = (8, 6)
MESH = pl.DeviceIdType.MESH
HALF_LOG2E = 0.5 * math.log2(math.e)
TWO_PI = 6.283185307179586


def over(n, body, init):
    if n <= 16:
        for i in range(n):
            init = body(i, init)
        return init
    return lax.fori_loop(0, n, body, init)


def densities(grid_col, rows_u, rows_v, rows_c, tiles, out_ref, first):
    n_config = rows_u.shape[0]
    grid = grid_col[...]

    def one_tile(t, carry):
        def term(k, acc):
            at = grid * rows_u[k, pl.ds(t, 1), :] + rows_v[k, pl.ds(t, 1), :]
            return acc + jnp.exp2(rows_c[k, pl.ds(t, 1), :] - at * at)

        acc = over(n_config, term, jnp.zeros(grid.shape, jnp.float32))
        column_at = pl.multiple_of((first + t) * LANES, LANES)
        out_ref[:, pl.ds(column_at, LANES)] = acc
        return carry

    lax.fori_loop(0, tiles, one_tile, 0)


def kernel(
    n_cfg, n_lat, own, spans,
    mode_ref, var_ref, weight_hbm, grid_hbm,
    density_ref, moments_ref, last_u, last_v, last_c, grid_col,
    stage, relay, landed, weights, norm, weight_ref, grid_ref, rows_u, rows_v, rows_c,
    small_sem, peer_sem, go_sem, rest_sem, pace_sem, load_sem, pass_sem, relay_sem, send_sem, recv_sem, wsend_sem, wrecv_sem,
):
    my_cfg = lax.axis_index("cfg")
    my_lat = lax.axis_index("lat")
    me = my_cfg * n_lat + my_lat
    n_group = n_lat // CORES
    group, core = my_lat // CORES, lax.rem(my_lat, CORES)
    per_group = n_cfg // n_group
    n_chunk = len(spans)

    def rows_of(chunk, until=None):
        start = 2 * own * spans[chunk][0]
        t, n = spans[chunk if until is None else until]
        return pl.ds(start, 2 * own * (t + n) - start)

    barrier = pltpu.get_barrier_semaphore()
    half_cfg = n_cfg // 2
    half = my_cfg // half_cfg
    gate = 1 - half
    is_gate = core == gate

    for step in range(1, n_group):
        peer = lax.rem(group + step, n_group) * CORES + jnp.where(half == 0, 0, core)
        pl.semaphore_signal(
            barrier, inc=1, device_id=(my_cfg, peer), device_id_type=MESH
        )

    def greet(i, carry):
        early = i < half_cfg
        mate = jnp.logical_and(i == my_cfg, jnp.logical_and(core != gate, half == 1))
        others = jnp.logical_and(i != my_cfg, jnp.logical_or(early, half == 0))
        mate = jnp.logical_or(
            mate, jnp.logical_and(i == my_cfg, jnp.logical_and(half == 0, core == 0))
        )

        @pl.when(jnp.logical_or(mate, others))
        def _():
            pl.semaphore_signal(
                barrier, inc=1,
                device_id=(i, group * CORES + jnp.where(early, 1, 0)), device_id_type=MESH,
            )
        return carry

    @pl.when(jnp.logical_and(half == 0, core == 1))
    def _():
        pl.semaphore_signal(
            barrier, inc=1, device_id=(my_cfg, group * CORES), device_id_type=MESH
        )

    over(n_cfg, greet, 0)

    for chunk in range(n_chunk):
        start, tiles = spans[chunk]
        n_row = own * tiles
        for step in list(range(1, n_group)) + [0]:
            to = lax.rem(group + step, n_group)
            for a, ref in enumerate((mode_ref, var_ref)):
                pltpu.make_async_copy(
                    ref.at[:, to, :, pl.ds(own * start, n_row)],
                    stage.at[to, :, :, pl.ds(2 * own * start + a * n_row, n_row)],
                    load_sem.at[step, min(chunk, 1)],
                ).start()
    small = [
        pltpu.make_async_copy(weight_hbm, weight_ref, small_sem.at[0]),
        pltpu.make_async_copy(grid_hbm, grid_ref, small_sem.at[1]),
    ]
    for copy in small:
        copy.start()

    peers = n_group - 1
    mate_id = (my_cfg, group * CORES + 1 - core)
    first_wait = jnp.where(
        half == 0, peers * CORES + 1,
        peers + jnp.where(is_gate, half_cfg * CORES + 1, 0),
    )

    @pl.when(jnp.logical_or(half == 1, core == 0))
    def _():
        pl.semaphore_wait(barrier, first_wait)

    @pl.when(half == 0)
    def _():
        @pl.when(core == 0)
        def _():
            pl.semaphore_signal(peer_sem, inc=1, device_id=mate_id, device_id_type=MESH)

        @pl.when(core != 0)
        def _():
            pl.semaphore_wait(peer_sem, 1)

    def spent(block, sem):
        pltpu.make_async_copy(block, block, sem).wait()

    def loaded(step, chunk):
        to = lax.rem(group + step, n_group)
        if chunk == 0:
            spent(stage.at[to, :, :, rows_of(0)], load_sem.at[step, 0])
        if chunk == 1:
            spent(stage.at[to, :, :, rows_of(1, n_chunk - 1)], load_sem.at[step, 1])

    def hop(chunk):
        for step in range(1, n_group):
            to = lax.rem(group + step, n_group)
            loaded(step, chunk)
            slot = n_group - step - 1
            pltpu.make_async_remote_copy(
                src_ref=stage.at[to, :, :, rows_of(chunk)],
                dst_ref=relay.at[slot, :, :, rows_of(chunk)],
                send_sem=pass_sem, recv_sem=relay_sem.at[slot, chunk],
                device_id=(my_cfg, to * CORES + core), device_id_type=MESH,
            ).start()

    for chunk in range(n_chunk):
        hop(chunk)

    @pl.when(jnp.logical_and(half == 0, is_gate))
    def _():
        pl.semaphore_wait(barrier, n_cfg * CORES - 1)

    @pl.when(is_gate)
    def _():
        pl.semaphore_signal(go_sem, inc=1, device_id=mate_id, device_id_type=MESH)

        @pl.when(half == 0)
        def _():
            for other in range(CORES):
                pl.semaphore_signal(
                    rest_sem, inc=1,
                    device_id=(my_cfg + half_cfg, group * CORES + other), device_id_type=MESH,
                )

    @pl.when(jnp.logical_not(is_gate))
    def _():
        pl.semaphore_wait(go_sem, 1)

    def target(origin, i):
        slot = (i // CORES) * n_lat + group * CORES + i % CORES
        flat = (origin * CORES + core) * n_cfg + slot
        return flat, (flat // n_lat, lax.rem(flat, n_lat))

    def send_weights(origin):
        def send(i, carry):
            flat, device = target(origin, i)

            @pl.when(flat == me)
            def _():
                pltpu.make_async_copy(weight_ref, weights.at[my_cfg], wrecv_sem).start()

            @pl.when(flat != me)
            def _():
                pltpu.make_async_remote_copy(
                    src_ref=weight_ref, dst_ref=weights.at[my_cfg],
                    send_sem=wsend_sem, recv_sem=wrecv_sem,
                    device_id=device, device_id_type=MESH,
                ).start()
            return carry

        over(per_group, send, 0)

    def send_blocks(origin, source, chunk, some=None):
        rows = rows_of(chunk)

        def send(i, carry):
            flat, device = target(origin, i)
            src = source.at[i // CORES, i % CORES, rows]
            dst = landed.at[my_cfg, rows]

            @pl.when(flat == me)
            def _():
                pltpu.make_async_copy(src, dst, recv_sem.at[chunk]).start()

            @pl.when(flat != me)
            def _():
                pltpu.make_async_remote_copy(
                    src_ref=src, dst_ref=dst,
                    send_sem=send_sem, recv_sem=recv_sem.at[chunk],
                    device_id=device, device_id_type=MESH,
                ).start()
            return carry

        if some is None:
            over(per_group, send, 0)
        else:
            lo, hi = (per_group * p // 2 for p in (some, some + 1))
            over(hi - lo, lambda i, carry: send(i + lo, carry), 0)

    def send_own(chunk, some=None):
        if some != 1:
            loaded(0, chunk)
        send_blocks(group, stage.at[group], chunk, some)

    def crosses(origin):
        return (origin * CORES + core) * 2 // n_lat != half

    def send_relayed(chunk):
        for step in range(1, n_group):
            origin = lax.rem(group + step, n_group)
            block = relay.at[step - 1, :, :, rows_of(chunk)]
            spent(block, relay_sem.at[step - 1, chunk])
            send_blocks(origin, relay.at[step - 1], chunk)

    own_first = crosses(group)

    def weights_where(first):
        for origin in range(n_group):
            @pl.when(crosses(origin) == first)
            def _():
                send_weights(origin)

    small[0].wait()
    weights_where(True)

    @pl.when(half == 0)
    def _():
        weights_where(False)

    @pl.when(half == 0)
    def _():
        for chunk in range(n_chunk):
            send_own(chunk)

    @pl.when(jnp.logical_and(half == 1, own_first))
    def _():
        for chunk in range(n_chunk + LEAD):
            if chunk < n_chunk:
                send_own(chunk, 0)
            if chunk >= LEAD:
                send_own(chunk - LEAD, 1)

    ahead = min(AHEAD, n_chunk)

    @pl.when(jnp.logical_not(own_first))
    def _():
        for chunk in range(ahead):
            send_relayed(chunk)

    @pl.when(half == 1)
    def _():
        pl.semaphore_wait(rest_sem, 1)
        weights_where(False)

        @pl.when(jnp.logical_not(own_first))
        def _():
            for chunk in range(n_chunk):
                send_own(chunk)

    @pl.when(own_first)
    def _():
        for chunk in range(ahead):
            send_relayed(chunk)

    relay_crosses = jnp.logical_not(own_first)
    for chunk in range(ahead, n_chunk):
        for which in range(2):
            if chunk == HOLD[which]:
                @pl.when(jnp.logical_and(relay_crosses, jnp.logical_and(half == which, core == 1)))
                def _():
                    pl.semaphore_wait(pace_sem, 1)

        send_relayed(chunk)

    for which in range(2):
        if HOLD[which] < n_chunk:
            @pl.when(jnp.logical_and(relay_crosses, jnp.logical_and(half == which, core == 0)))
            def _():
                pl.semaphore_signal(pace_sem, inc=1, device_id=mate_id, device_id_type=MESH)

    small[1].wait()
    points = grid_ref.shape[1]
    on_diagonal = lax.broadcasted_iota(jnp.int32, (points, points), 0) == lax.broadcasted_iota(
        jnp.int32, (points, points), 1
    )
    column = jnp.sum(jnp.where(on_diagonal, grid_ref[...], 0.0), axis=1, keepdims=True)
    grid_col[...] = jnp.broadcast_to(column, (points, LANES))

    pltpu.make_async_copy(weights, weights, wrecv_sem).wait()
    total = jnp.zeros((1, 1), jnp.float32)
    for c in range(n_cfg):
        total = total + jnp.sum(weights[c], axis=1, keepdims=True)
    for c in range(n_cfg):
        scaled = weights[c] / total
        for j in range(own):
            norm[c * own + j] = jnp.broadcast_to(scaled[:, j:j + 1], (1, LANES))

    for chunk in range(n_chunk):
        start, tiles = spans[chunk]
        base = 2 * own * start
        n_row = own * tiles
        shape = (tiles, LANES)
        arrived = landed.at[:, rows_of(chunk)]
        pltpu.make_async_copy(arrived, arrived, recv_sem.at[chunk]).wait()

        def value(c, a, j):
            return landed[c, pl.ds(base + a * n_row + j, tiles, stride=own), :]

        def add_mode(c, acc):
            for j in range(own):
                acc = acc + norm[c * own + j] * value(c, 0, j)
            return acc

        centre = over(n_cfg, add_mode, jnp.zeros(shape, jnp.float32))

        def add_var(c, acc):
            for j in range(own):
                off = value(c, 0, j) - centre
                acc = acc + norm[c * own + j] * (value(c, 1, j) + off * off)
            return acc

        spread = jnp.sqrt(over(n_cfg, add_var, jnp.zeros(shape, jnp.float32)))
        moments_ref[pl.ds(2 * start, tiles, stride=2), :] = centre
        moments_ref[pl.ds(2 * start + 1, tiles, stride=2), :] = spread

        final = chunk == n_chunk - 1
        to_u, to_v, to_c = (last_u, last_v, last_c) if final else (rows_u, rows_v, rows_c)

        def prepare(c, carry):
            for j in range(own):
                k = c * own + j
                root = lax.rsqrt(value(c, 1, j))
                scale = root * math.sqrt(HALF_LOG2E)
                to_u[k, pl.ds(0, tiles)] = spread * scale
                to_v[k, pl.ds(0, tiles)] = (centre - value(c, 0, j)) * scale
                to_c[k, pl.ds(0, tiles)] = jnp.log2(
                    norm[k] * spread * root * (1.0 / math.sqrt(TWO_PI))
                )
            return carry

        over(n_cfg, prepare, 0)

        if not final:
            densities(
                grid_col, rows_u, rows_v, rows_c, tiles, density_ref, start
            )

    spent(stage.at[pl.ds(0, n_group - 1)], pass_sem)
    for kept, n in ((lax.rem(me // n_cfg, CORES) == core, n_cfg - 1),
                    (lax.rem(me // n_cfg, CORES) != core, n_cfg)):
        @pl.when(kept)
        def _():
            spent(weights.at[pl.ds(0, n)], wsend_sem)
            spent(landed.at[pl.ds(0, n)], send_sem)


def finish(
    tiles,
    done_ref, made_ref, rows_u, rows_v, rows_c, grid_col,
    density_ref, moments_ref,
    last, sems,
):
    early = done_ref.shape[1]
    copies = [
        pltpu.make_async_copy(done_ref, density_ref.at[:, pl.ds(0, early)], sems.at[0]),
        pltpu.make_async_copy(made_ref, moments_ref, sems.at[1]),
    ]
    for copy in copies:
        copy.start()
    densities(grid_col, rows_u, rows_v, rows_c, tiles, last, 0)
    copies.append(
        pltpu.make_async_copy(
            last, density_ref.at[:, pl.ds(early, tiles * LANES)], sems.at[2]
        )
    )
    copies[2].start()
    for copy in copies:
        copy.wait()


def interleave(block, n_cfg, n_lat):
    own, columns = block.shape
    rows = block.reshape(own, columns // LANES, LANES).transpose(1, 0, 2)
    n_row = columns * own // (LANES * n_cfg)
    return rows.reshape(n_cfg // n_lat, n_lat // CORES, CORES, n_row, LANES)


def per_device(latent_mode, latent_var, config_weight, grid_offset):
    n_cfg = lax.axis_size("cfg")
    n_lat = lax.axis_size("lat")
    own, columns = latent_mode.shape
    lat_dev = columns // n_cfg
    points = grid_offset.shape[0]
    unit = lat_dev // (LANES * sum(UNITS))
    spans = []
    for n in UNITS:
        spans.append((sum(s[1] for s in spans), n * unit))
    most, last = max(n for _, n in spans[:-1]), spans[-1][1]
    n_chunk = len(spans)
    n_config = own * n_cfg
    n_group = n_lat // CORES
    n_row = 2 * own * lat_dev // LANES
    n_a = n_cfg // n_lat
    f32 = jnp.float32
    hbm = pl.BlockSpec(memory_space=pl.ANY)
    vmem = pl.BlockSpec(memory_space=pltpu.VMEM)
    early = lat_dev - last * LANES
    interleaved = (2 * lat_dev // LANES, LANES)
    dma = pltpu.SemaphoreType.DMA
    parts = pl.pallas_call(
        functools.partial(kernel, n_cfg, n_lat, own, spans),
        out_shape=(
            pltpu.VMEM((points, early), f32),
            pltpu.VMEM(interleaved, f32),
            pltpu.VMEM((n_config, last, LANES), f32),
            pltpu.VMEM((n_config, last, LANES), f32),
            pltpu.VMEM((n_config, last, LANES), f32),
            pltpu.VMEM((points, LANES), f32),
        ),
        in_specs=[hbm] * 4,
        out_specs=(vmem,) * 6,
        scratch_shapes=[
            pltpu.VMEM((n_group, n_a, CORES, n_row, LANES), f32),
            pltpu.VMEM((n_group - 1, n_a, CORES, n_row, LANES), f32),
            pltpu.VMEM((n_cfg, n_row, LANES), f32),
            pltpu.VMEM((n_cfg, 1, own), f32),
            pltpu.VMEM((n_config, 1, LANES), f32),
            pltpu.VMEM((1, own), f32),
            pltpu.VMEM((1, points), f32),
            pltpu.VMEM((n_config, most, LANES), f32),
            pltpu.VMEM((n_config, most, LANES), f32),
            pltpu.VMEM((n_config, most, LANES), f32),
            dma((2,)),
            pltpu.SemaphoreType.REGULAR,
            pltpu.SemaphoreType.REGULAR,
            pltpu.SemaphoreType.REGULAR,
            pltpu.SemaphoreType.REGULAR,
            dma((n_group, 2)),
            dma,
            dma((n_group - 1, n_chunk)),
            dma,
            dma((n_chunk,)),
            dma,
            dma,
        ],
        compiler_params=pltpu.CompilerParams(collective_id=0, has_side_effects=True),
    )(
        interleave(latent_mode, n_cfg, n_lat),
        interleave(latent_var, n_cfg, n_lat),
        config_weight.reshape(1, own),
        grid_offset.reshape(1, points),
    )
    density, moments = pl.pallas_call(
        functools.partial(finish, last),
        out_shape=(
            jax.ShapeDtypeStruct((points, lat_dev), f32),
            jax.ShapeDtypeStruct(interleaved, f32),
        ),
        in_specs=[vmem] * 6,
        out_specs=(hbm, hbm),
        scratch_shapes=[
            pltpu.VMEM((points, last * LANES), f32),
            dma((3,)),
        ],
    )(*(pltpu.with_memory_space_constraint(part, pltpu.VMEM) for part in parts))
    moments = moments.reshape(lat_dev // LANES, 2, LANES).transpose(1, 0, 2).reshape(2, lat_dev)
    return (density, moments)


def solution(mesh):
    return jax.shard_map(
        per_device,
        mesh=mesh,
        in_specs=(P("cfg", "lat"), P("cfg", "lat"), P("cfg"), P()),
        out_specs=(P(None, ("cfg", "lat")), P(None, ("cfg", "lat"))),
        check_vma=False,
    )
```

```python
import functools
import math

import jax
import jax.numpy as jnp
from jax import lax
from jax.experimental import pallas as pl
from jax.experimental.pallas import tpu as pltpu
from jax.sharding import PartitionSpec as P

LANES = 128
CORES = 2
UNITS = (1, 1, 1, 1, 1, 1, 1, 1)
AHEAD = 6
LEAD = 4
HOLD = (8, 6)
MESH = pl.DeviceIdType.MESH
HALF_LOG2E = 0.5 * math.log2(math.e)
TWO_PI = 6.283185307179586


def over(n, body, init):
    if n <= 16:
        for i in range(n):
            init = body(i, init)
        return init
    return lax.fori_loop(0, n, body, init)


def densities(grid_col, rows_u, rows_v, rows_c, tiles, out_ref, first):
    n_config = rows_u.shape[0]
    grid = grid_col[...]

    def one_tile(t, carry):
        def term(k, acc):
            at = grid * rows_u[k, pl.ds(t, 1), :] + rows_v[k, pl.ds(t, 1), :]
            return acc + jnp.exp2(rows_c[k, pl.ds(t, 1), :] - at * at)

        acc = over(n_config, term, jnp.zeros(grid.shape, jnp.float32))
        column_at = pl.multiple_of((first + t) * LANES, LANES)
        out_ref[:, pl.ds(column_at, LANES)] = acc
        return carry

    lax.fori_loop(0, tiles, one_tile, 0)


def kernel(
    n_cfg, n_lat, own, spans,
    mode_ref, var_ref, weight_hbm, grid_hbm,
    density_ref, moments_ref, last_u, last_v, last_c, grid_col,
    stage, relay, landed, weights, norm, weight_ref, grid_ref, rows_u, rows_v, rows_c,
    small_sem, peer_sem, go_sem, rest_sem, pace_sem, load_sem, pass_sem, relay_sem, send_sem, recv_sem, wsend_sem, wrecv_sem,
):
    my_cfg = lax.axis_index("cfg")
    my_lat = lax.axis_index("lat")
    me = my_cfg * n_lat + my_lat
    n_group = n_lat // CORES
    group, core = my_lat // CORES, lax.rem(my_lat, CORES)
    per_group = n_cfg // n_group
    n_chunk = len(spans)

    def rows_of(chunk, until=None):
        start = 2 * own * spans[chunk][0]
        t, n = spans[chunk if until is None else until]
        return pl.ds(start, 2 * own * (t + n) - start)

    barrier = pltpu.get_barrier_semaphore()
    half_cfg = n_cfg // 2
    half = my_cfg // half_cfg
    gate = 1 - half
    is_gate = core == gate

    for step in range(1, n_group):
        peer = lax.rem(group + step, n_group) * CORES + jnp.where(half == 0, 0, core)
        pl.semaphore_signal(
            barrier, inc=1, device_id=(my_cfg, peer), device_id_type=MESH
        )

    def greet(i, carry):
        early = i < half_cfg
        mate = jnp.logical_and(i == my_cfg, jnp.logical_and(core != gate, half == 1))
        others = jnp.logical_and(i != my_cfg, jnp.logical_or(early, half == 0))
        mate = jnp.logical_or(
            mate, jnp.logical_and(i == my_cfg, jnp.logical_and(half == 0, core == 0))
        )

        @pl.when(jnp.logical_or(mate, others))
        def _():
            pl.semaphore_signal(
                barrier, inc=1,
                device_id=(i, group * CORES + jnp.where(early, 1, 0)), device_id_type=MESH,
            )
        return carry

    @pl.when(jnp.logical_and(half == 0, core == 1))
    def _():
        pl.semaphore_signal(
            barrier, inc=1, device_id=(my_cfg, group * CORES), device_id_type=MESH
        )

    over(n_cfg, greet, 0)

    for chunk in range(n_chunk):
        start, tiles = spans[chunk]
        n_row = own * tiles
        for step in list(range(1, n_group)) + [0]:
            to = lax.rem(group + step, n_group)
            for a, ref in enumerate((mode_ref, var_ref)):
                pltpu.make_async_copy(
                    ref.at[:, to, :, pl.ds(own * start, n_row)],
                    stage.at[to, :, :, pl.ds(2 * own * start + a * n_row, n_row)],
                    load_sem.at[step, min(chunk, 1)],
                ).start()
    small = [
        pltpu.make_async_copy(weight_hbm, weight_ref, small_sem.at[0]),
        pltpu.make_async_copy(grid_hbm, grid_ref, small_sem.at[1]),
    ]
    for copy in small:
        copy.start()

    peers = n_group - 1
    mate_id = (my_cfg, group * CORES + 1 - core)
    first_wait = jnp.where(
        half == 0, peers * CORES + 1,
        peers + jnp.where(is_gate, half_cfg * CORES + 1, 0),
    )

    @pl.when(jnp.logical_or(half == 1, core == 0))
    def _():
        pl.semaphore_wait(barrier, first_wait)

    @pl.when(half == 0)
    def _():
        @pl.when(core == 0)
        def _():
            pl.semaphore_signal(peer_sem, inc=1, device_id=mate_id, device_id_type=MESH)

        @pl.when(core != 0)
        def _():
            pl.semaphore_wait(peer_sem, 1)

    def spent(block, sem):
        pltpu.make_async_copy(block, block, sem).wait()

    def loaded(step, chunk):
        to = lax.rem(group + step, n_group)
        if chunk == 0:
            spent(stage.at[to, :, :, rows_of(0)], load_sem.at[step, 0])
        if chunk == 1:
            spent(stage.at[to, :, :, rows_of(1, n_chunk - 1)], load_sem.at[step, 1])

    def hop(chunk):
        for step in range(1, n_group):
            to = lax.rem(group + step, n_group)
            loaded(step, chunk)
            slot = n_group - step - 1
            pltpu.make_async_remote_copy(
                src_ref=stage.at[to, :, :, rows_of(chunk)],
                dst_ref=relay.at[slot, :, :, rows_of(chunk)],
                send_sem=pass_sem, recv_sem=relay_sem.at[slot, chunk],
                device_id=(my_cfg, to * CORES + core), device_id_type=MESH,
            ).start()

    for chunk in range(n_chunk):
        hop(chunk)

    @pl.when(jnp.logical_and(half == 0, is_gate))
    def _():
        pl.semaphore_wait(barrier, n_cfg * CORES - 1)

    @pl.when(is_gate)
    def _():
        pl.semaphore_signal(go_sem, inc=1, device_id=mate_id, device_id_type=MESH)

        @pl.when(half == 0)
        def _():
            for other in range(CORES):
                pl.semaphore_signal(
                    rest_sem, inc=1,
                    device_id=(my_cfg + half_cfg, group * CORES + other), device_id_type=MESH,
                )

    @pl.when(jnp.logical_not(is_gate))
    def _():
        pl.semaphore_wait(go_sem, 1)

    def target(origin, i):
        slot = (i // CORES) * n_lat + group * CORES + i % CORES
        flat = (origin * CORES + core) * n_cfg + slot
        return flat, (flat // n_lat, lax.rem(flat, n_lat))

    def send_weights(origin):
        def send(i, carry):
            flat, device = target(origin, i)

            @pl.when(flat == me)
            def _():
                pltpu.make_async_copy(weight_ref, weights.at[my_cfg], wrecv_sem).start()

            @pl.when(flat != me)
            def _():
                pltpu.make_async_remote_copy(
                    src_ref=weight_ref, dst_ref=weights.at[my_cfg],
                    send_sem=wsend_sem, recv_sem=wrecv_sem,
                    device_id=device, device_id_type=MESH,
                ).start()
            return carry

        over(per_group, send, 0)

    def send_blocks(origin, source, chunk, some=None):
        rows = rows_of(chunk)

        def send(i, carry):
            flat, device = target(origin, i)
            src = source.at[i // CORES, i % CORES, rows]
            dst = landed.at[my_cfg, rows]

            @pl.when(flat == me)
            def _():
                pltpu.make_async_copy(src, dst, recv_sem.at[chunk]).start()

            @pl.when(flat != me)
            def _():
                pltpu.make_async_remote_copy(
                    src_ref=src, dst_ref=dst,
                    send_sem=send_sem, recv_sem=recv_sem.at[chunk],
                    device_id=device, device_id_type=MESH,
                ).start()
            return carry

        if some is None:
            over(per_group, send, 0)
        else:
            lo, hi = (per_group * p // 2 for p in (some, some + 1))
            over(hi - lo, lambda i, carry: send(i + lo, carry), 0)

    def send_own(chunk, some=None):
        if some != 1:
            loaded(0, chunk)
        send_blocks(group, stage.at[group], chunk, some)

    def crosses(origin):
        return (origin * CORES + core) * 2 // n_lat != half

    def send_relayed(chunk):
        for step in range(1, n_group):
            origin = lax.rem(group + step, n_group)
            block = relay.at[step - 1, :, :, rows_of(chunk)]
            spent(block, relay_sem.at[step - 1, chunk])
            send_blocks(origin, relay.at[step - 1], chunk)

    own_first = crosses(group)

    def weights_where(first):
        for origin in range(n_group):
            @pl.when(crosses(origin) == first)
            def _():
                send_weights(origin)

    small[0].wait()
    weights_where(True)

    @pl.when(half == 0)
    def _():
        weights_where(False)

    @pl.when(half == 0)
    def _():
        for chunk in range(n_chunk):
            send_own(chunk)

    @pl.when(jnp.logical_and(half == 1, own_first))
    def _():
        for chunk in range(n_chunk + LEAD):
            if chunk < n_chunk:
                send_own(chunk, 0)
            if chunk >= LEAD:
                send_own(chunk - LEAD, 1)

    ahead = min(AHEAD, n_chunk)

    @pl.when(jnp.logical_not(own_first))
    def _():
        for chunk in range(ahead):
            send_relayed(chunk)

    @pl.when(half == 1)
    def _():
        pl.semaphore_wait(rest_sem, 1)
        weights_where(False)

        @pl.when(jnp.logical_not(own_first))
        def _():
            for chunk in range(n_chunk):
                send_own(chunk)

    @pl.when(own_first)
    def _():
        for chunk in range(ahead):
            send_relayed(chunk)

    relay_crosses = jnp.logical_not(own_first)
    for chunk in range(ahead, n_chunk):
        for which in range(2):
            if chunk == HOLD[which]:
                @pl.when(jnp.logical_and(relay_crosses, jnp.logical_and(half == which, core == 1)))
                def _():
                    pl.semaphore_wait(pace_sem, 1)

        send_relayed(chunk)

    for which in range(2):
        if HOLD[which] < n_chunk:
            @pl.when(jnp.logical_and(relay_crosses, jnp.logical_and(half == which, core == 0)))
            def _():
                pl.semaphore_signal(pace_sem, inc=1, device_id=mate_id, device_id_type=MESH)

    small[1].wait()
    points = grid_ref.shape[1]
    on_diagonal = lax.broadcasted_iota(jnp.int32, (points, points), 0) == lax.broadcasted_iota(
        jnp.int32, (points, points), 1
    )
    column = jnp.sum(jnp.where(on_diagonal, grid_ref[...], 0.0), axis=1, keepdims=True)
    grid_col[...] = jnp.broadcast_to(column, (points, LANES))

    pltpu.make_async_copy(weights, weights, wrecv_sem).wait()
    total = jnp.zeros((1, 1), jnp.float32)
    for c in range(n_cfg):
        total = total + jnp.sum(weights[c], axis=1, keepdims=True)
    for c in range(n_cfg):
        scaled = weights[c] / total
        for j in range(own):
            norm[c * own + j] = jnp.broadcast_to(scaled[:, j:j + 1], (1, LANES))

    for chunk in range(n_chunk):
        start, tiles = spans[chunk]
        base = 2 * own * start
        n_row = own * tiles
        shape = (tiles, LANES)
        arrived = landed.at[:, rows_of(chunk)]
        pltpu.make_async_copy(arrived, arrived, recv_sem.at[chunk]).wait()

        def value(c, a, j):
            return landed[c, pl.ds(base + a * n_row + j, tiles, stride=own), :]

        def add_mode(c, acc):
            for j in range(own):
                acc = acc + norm[c * own + j] * value(c, 0, j)
            return acc

        centre = over(n_cfg, add_mode, jnp.zeros(shape, jnp.float32))

        def add_var(c, acc):
            for j in range(own):
                off = value(c, 0, j) - centre
                acc = acc + norm[c * own + j] * (value(c, 1, j) + off * off)
            return acc

        spread = jnp.sqrt(over(n_cfg, add_var, jnp.zeros(shape, jnp.float32)))
        moments_ref[pl.ds(2 * start, tiles, stride=2), :] = centre
        moments_ref[pl.ds(2 * start + 1, tiles, stride=2), :] = spread

        final = chunk == n_chunk - 1
        to_u, to_v, to_c = (last_u, last_v, last_c) if final else (rows_u, rows_v, rows_c)

        def prepare(c, carry):
            for j in range(own):
                k = c * own + j
                root = lax.rsqrt(value(c, 1, j))
                scale = root * math.sqrt(HALF_LOG2E)
                to_u[k, pl.ds(0, tiles)] = spread * scale
                to_v[k, pl.ds(0, tiles)] = (centre - value(c, 0, j)) * scale
                to_c[k, pl.ds(0, tiles)] = jnp.log2(
                    norm[k] * spread * root * (1.0 / math.sqrt(TWO_PI))
                )
            return carry

        over(n_cfg, prepare, 0)

        if not final:
            densities(
                grid_col, rows_u, rows_v, rows_c, tiles, density_ref, start
            )

    spent(stage.at[pl.ds(0, n_group - 1)], pass_sem)
    for kept, n in ((lax.rem(me // n_cfg, CORES) == core, n_cfg - 1),
                    (lax.rem(me // n_cfg, CORES) != core, n_cfg)):
        @pl.when(kept)
        def _():
            spent(weights.at[pl.ds(0, n)], wsend_sem)
            spent(landed.at[pl.ds(0, n)], send_sem)


def finish(
    tiles,
    done_ref, made_ref, rows_u, rows_v, rows_c, grid_col,
    density_ref, moments_ref,
    last, sems,
):
    early = done_ref.shape[1]
    copies = [
        pltpu.make_async_copy(done_ref, density_ref.at[:, pl.ds(0, early)], sems.at[0]),
        pltpu.make_async_copy(made_ref, moments_ref, sems.at[1]),
    ]
    for copy in copies:
        copy.start()
    densities(grid_col, rows_u, rows_v, rows_c, tiles, last, 0)
    copies.append(
        pltpu.make_async_copy(
            last, density_ref.at[:, pl.ds(early, tiles * LANES)], sems.at[2]
        )
    )
    copies[2].start()
    for copy in copies:
        copy.wait()


def interleave(block, n_cfg, n_lat):
    own, columns = block.shape
    rows = block.reshape(own, columns // LANES, LANES).transpose(1, 0, 2)
    n_row = columns * own // (LANES * n_cfg)
    return rows.reshape(n_cfg // n_lat, n_lat // CORES, CORES, n_row, LANES)


def per_device(latent_mode, latent_var, config_weight, grid_offset):
    n_cfg = lax.axis_size("cfg")
    n_lat = lax.axis_size("lat")
    own, columns = latent_mode.shape
    lat_dev = columns // n_cfg
    points = grid_offset.shape[0]
    unit = lat_dev // (LANES * sum(UNITS))
    spans = []
    for n in UNITS:
        spans.append((sum(s[1] for s in spans), n * unit))
    most, last = max(n for _, n in spans[:-1]), spans[-1][1]
    n_chunk = len(spans)
    n_config = own * n_cfg
    n_group = n_lat // CORES
    n_row = 2 * own * lat_dev // LANES
    n_a = n_cfg // n_lat
    f32 = jnp.float32
    hbm = pl.BlockSpec(memory_space=pl.ANY)
    vmem = pl.BlockSpec(memory_space=pltpu.VMEM)
    early = lat_dev - last * LANES
    interleaved = (2 * lat_dev // LANES, LANES)
    dma = pltpu.SemaphoreType.DMA
    parts = pl.pallas_call(
        functools.partial(kernel, n_cfg, n_lat, own, spans),
        out_shape=(
            pltpu.VMEM((points, early), f32),
            pltpu.VMEM(interleaved, f32),
            pltpu.VMEM((n_config, last, LANES), f32),
            pltpu.VMEM((n_config, last, LANES), f32),
            pltpu.VMEM((n_config, last, LANES), f32),
            pltpu.VMEM((points, LANES), f32),
        ),
        in_specs=[hbm] * 4,
        out_specs=(vmem,) * 6,
        scratch_shapes=[
            pltpu.VMEM((n_group, n_a, CORES, n_row, LANES), f32),
            pltpu.VMEM((n_group - 1, n_a, CORES, n_row, LANES), f32),
            pltpu.VMEM((n_cfg, n_row, LANES), f32),
            pltpu.VMEM((n_cfg, 1, own), f32),
            pltpu.VMEM((n_config, 1, LANES), f32),
            pltpu.VMEM((1, own), f32),
            pltpu.VMEM((1, points), f32),
            pltpu.VMEM((n_config, most, LANES), f32),
            pltpu.VMEM((n_config, most, LANES), f32),
            pltpu.VMEM((n_config, most, LANES), f32),
            dma((2,)),
            pltpu.SemaphoreType.REGULAR,
            pltpu.SemaphoreType.REGULAR,
            pltpu.SemaphoreType.REGULAR,
            pltpu.SemaphoreType.REGULAR,
            dma((n_group, 2)),
            dma,
            dma((n_group - 1, n_chunk)),
            dma,
            dma((n_chunk,)),
            dma,
            dma,
        ],
        compiler_params=pltpu.CompilerParams(collective_id=0, has_side_effects=True),
    )(
        interleave(latent_mode, n_cfg, n_lat),
        interleave(latent_var, n_cfg, n_lat),
        config_weight.reshape(1, own),
        grid_offset.reshape(1, points),
    )
    density, moments = pl.pallas_call(
        functools.partial(finish, last),
        out_shape=(
            jax.ShapeDtypeStruct((points, lat_dev), f32),
            jax.ShapeDtypeStruct(interleaved, f32),
        ),
        in_specs=[vmem] * 6,
        out_specs=(hbm, hbm),
        scratch_shapes=[
            pltpu.VMEM((points, last * LANES), f32),
            dma((3,)),
        ],
    )(*(pltpu.with_memory_space_constraint(part, pltpu.VMEM) for part in parts))
    moments = moments.reshape(lat_dev // LANES, 2, LANES).transpose(1, 0, 2).reshape(2, lat_dev)
    return (density, moments)


def solution(mesh):
    return jax.shard_map(
        per_device,
        mesh=mesh,
        in_specs=(P("cfg", "lat"), P("cfg", "lat"), P("cfg"), P()),
        out_specs=(P(None, ("cfg", "lat")), P(None, ("cfg", "lat"))),
        check_vma=False,
    )
```
